16 devices in a mesh: dp: 2 (over z), vp: 8 (over y, x, core).
Axes of the slice: x: 2, y: 2, z: 2, core: 2. Of those that a mesh axis runs over, the one named last changes fastest.
Arguments:
- hidden: bfloat16 [2048, 512], P('dp')
- norm_scale: float32 [512], replicated
- w_out: bfloat16 [512, 250112], P(None, 'vp')
- targets: int32 [2048], P('dp')
- weights: float32 [2048], P('dp')
Outputs:
- output 1: float32 [], replicated
- output 2: bfloat16 [2048, 512], P('dp')
- output 3: float32 [512, 250112], P(None, 'vp')
- output 4: float32 [512], replicated
All inputs are finite; a program needn't handle non-finite values.
Results may differ from the reference program's by a relative error of at most 0.001.
Values sent between devices are 32-bit elements.
A program may use at most 1 GiB of HBM per device.

```python
import jax
import jax.numpy as jnp
from jax import lax

TOKENS_DEV = 1024
DP_SIZE = 2
D_MODEL = 512
VOCAB_SIZE = 250112
BLOCK_ROWS = 128
EPS = 1e-6
TOTAL_TOKENS = TOKENS_DEV * DP_SIZE


def setup_inputs(seed: int = 0) -> dict:
    key = jax.random.key(seed)
    k_hid, k_scale, k_wout, k_col, k_tgt, k_pad = jax.random.split(key, 6)
    ramp = jnp.arange(VOCAB_SIZE, dtype=jnp.float32) / VOCAB_SIZE
    col_scale = 0.6 + 1.2 * ramp + 0.3 * jax.random.uniform(k_col, (VOCAB_SIZE,), jnp.float32)
    w_full = jax.random.normal(k_wout, (D_MODEL, VOCAB_SIZE), jnp.float32) * (col_scale * D_MODEL ** -0.5)
    targets = jax.random.randint(k_tgt, (TOTAL_TOKENS,), 0, VOCAB_SIZE, dtype=jnp.int32)
    signal = 4.0 * jnp.take(w_full, targets, axis=1).T / col_scale[targets][:, None]
    hidden = jax.random.normal(k_hid, (TOTAL_TOKENS, D_MODEL), jnp.float32) + signal
    norm_scale = 0.8 + 0.4 * jax.random.uniform(k_scale, (D_MODEL,), jnp.float32)
    pad_counts = jax.random.randint(k_pad, (DP_SIZE,), TOKENS_DEV // 10, 3 * TOKENS_DEV // 10 + 1, dtype=jnp.int32)
    positions = jnp.arange(TOKENS_DEV, dtype=jnp.int32)
    valid = positions[None, :] < (TOKENS_DEV - pad_counts)[:, None]
    weights = valid.astype(jnp.float32).reshape(TOTAL_TOKENS)
    return {'hidden': hidden.astype(jnp.bfloat16), 'norm_scale': norm_scale, 'w_out': w_full.astype(jnp.bfloat16), 'targets': targets, 'weights': weights}


def rms_norm(h_float, norm_scale):
    mean_sq = jnp.mean(h_float * h_float, axis=-1, keepdims=True)
    return h_float * lax.rsqrt(mean_sq + EPS) * norm_scale


def reference(hidden, norm_scale, w_out, targets, weights):
    w_total = jnp.sum(weights)
    vocab_ids = jnp.arange(VOCAB_SIZE, dtype=jnp.int32)
    num_blocks = TOTAL_TOKENS // BLOCK_ROWS
    h_blocks = hidden.reshape(num_blocks, BLOCK_ROWS, D_MODEL)
    t_blocks = targets.reshape(num_blocks, BLOCK_ROWS)
    wt_blocks = weights.reshape(num_blocks, BLOCK_ROWS)

    def body(carry, blk):
        grad_w, loss_sum, grad_scale = carry
        h_blk, t_blk, wt_blk = blk
        normed, norm_vjp = jax.vjp(rms_norm, h_blk.astype(jnp.float32), norm_scale)
        h_norm = normed.astype(jnp.bfloat16)
        logits = jnp.dot(h_norm, w_out, preferred_element_type=jnp.float32)
        row_max = jnp.max(logits, axis=-1, keepdims=True)
        log_norm = row_max + jnp.log(jnp.sum(jnp.exp(logits - row_max), axis=-1, keepdims=True))
        is_target = vocab_ids[None, :] == t_blk[:, None]
        tgt_logit = jnp.sum(jnp.where(is_target, logits, 0.0), axis=-1)
        loss_sum = loss_sum + jnp.sum(wt_blk * (log_norm[:, 0] - tgt_logit))
        tok_coef = (wt_blk / w_total)[:, None]
        grad_logits = (tok_coef * jnp.exp(logits - log_norm) - jnp.where(is_target, tok_coef, 0.0)).astype(jnp.bfloat16)
        grad_hn = jnp.dot(grad_logits, w_out.T, preferred_element_type=jnp.float32)
        grad_w = grad_w + jnp.dot(h_norm.T, grad_logits, preferred_element_type=jnp.float32)
        grad_h, grad_s = norm_vjp(grad_hn)
        return (grad_w, loss_sum, grad_scale + grad_s), grad_h.astype(jnp.bfloat16)

    init = (jnp.zeros((D_MODEL, VOCAB_SIZE), jnp.float32), jnp.zeros((), jnp.float32), jnp.zeros((D_MODEL,), jnp.float32))
    (grad_w, loss_sum, grad_scale), grad_h = lax.scan(body, init, (h_blocks, t_blocks, wt_blocks))
    return (loss_sum / w_total, grad_h.reshape(TOTAL_TOKENS, D_MODEL), grad_w, grad_scale)
```

```python
import functools

import jax
import jax.numpy as jnp
from jax import lax
from jax.experimental import pallas as pl
from jax.experimental.pallas import tpu as pltpu
from jax.sharding import PartitionSpec as P

EPS = 1e-6
SUB = 8
BLOCK_V = 768
CHUNK = 512
GROUP = 64
FIRST = 22
TN = (((0,), (0,)), ((), ()))


def stats_kernel(vocab, hnt_ref, w_ref, out_ref, m_ref, s_ref):
    i = pl.program_id(0)
    last = pl.num_programs(0) - 1
    tokens = hnt_ref.shape[1]

    @pl.when(i == 0)
    def _():
        m_ref[...] = jnp.full(m_ref.shape, -jnp.inf, jnp.float32)
        s_ref[...] = jnp.zeros(s_ref.shape, jnp.float32)

    def block(rows):
        for c in range(0, tokens, CHUNK):
            cols = pl.ds(c, CHUNK)
            z = jnp.dot(w_ref[:rows, :], hnt_ref[:, cols], preferred_element_type=jnp.float32)
            m, s = m_ref[:, cols], s_ref[:, cols]
            for r in range(0, rows, GROUP):
                n = min(GROUP, rows - r)
                part = z[r:r + n].reshape(n // SUB, SUB, CHUNK)
                m_new = jnp.maximum(m, jnp.max(part, axis=0))
                s = s * jnp.exp(m - m_new) + jnp.sum(jnp.exp(part - m_new[None]), axis=0)
                m = m_new
            m_ref[:, cols] = m
            s_ref[:, cols] = s

    @pl.when(i < last)
    def _():
        block(BLOCK_V)

    @pl.when(i == last)
    def _():
        block(vocab - (vocab - 1) // BLOCK_V * BLOCK_V)
        top = jnp.max(m_ref[...], axis=0, keepdims=True)
        out_ref[0:1, :] = top
        out_ref[1:2, :] = jnp.sum(s_ref[...] * jnp.exp(m_ref[...] - top), axis=0, keepdims=True)


def zero_tail(vocab, w_ref, wz_ref, is_last):
    tail = vocab - (vocab - 1) // BLOCK_V * BLOCK_V
    wz_ref[...] = w_ref[...]

    @pl.when(is_last)
    def _():
        wz_ref[tail:, :] = jnp.zeros((BLOCK_V - tail, wz_ref.shape[1]), jnp.bfloat16)


def softmax_grad(step, wz_ref, hnt_ref, tok_ref, base, g_ref, zt_ref=None):
    shape = (BLOCK_V // SUB, SUB, CHUNK)
    first_row = (lax.broadcasted_iota(jnp.int32, shape, 0) * SUB).astype(jnp.float32)
    sub = lax.broadcasted_iota(jnp.int32, shape[1:], 0)
    row0 = (sub + step * BLOCK_V).astype(jnp.float32)
    for c in range(0, hnt_ref.shape[1], CHUNK):
        cols, toks = pl.ds(c, CHUNK), pl.ds(base + c, CHUNK)
        z = jnp.dot(wz_ref[...], hnt_ref[:, cols], preferred_element_type=jnp.float32).reshape(shape)
        hit = (tok_ref[2 * SUB:, toks] - row0)[None] == first_row
        g = jnp.exp(z - tok_ref[:SUB, toks][None]) - jnp.where(hit, tok_ref[SUB:2 * SUB, toks][None], 0.0)
        g_ref[:, cols] = g.reshape(BLOCK_V, CHUNK).astype(jnp.bfloat16)
        if zt_ref is not None:
            zt_ref[:, cols] += jnp.sum(jnp.where(hit, z, 0.0), axis=0)


def first_kernel(vocab, hn_a_ref, hn_b_ref, hnt_a_ref, hnt_b_ref, w_ref, tok_ref, dw_ref, x_ref, g_out_ref, wz_ref, ga_ref, gb_ref):
    i = pl.program_id(0)
    width, own = hnt_a_ref.shape
    dhnt_ref = x_ref.at[:width]
    zt_ref = x_ref.at[width:]

    @pl.when(i == 0)
    def _():
        x_ref[...] = jnp.zeros(x_ref.shape, jnp.float32)

    zero_tail(vocab, w_ref, wz_ref, i == pl.num_programs(0) - 1)

    def own_part(g_ref):
        softmax_grad(i, wz_ref, hnt_a_ref, tok_ref, 0, g_ref, zt_ref)
        dhnt_ref[...] += lax.dot_general(wz_ref[...], g_ref[...], TN, preferred_element_type=jnp.float32)

    @pl.when(i < FIRST)
    def _():
        own_part(ga_ref)
        softmax_grad(i, wz_ref, hnt_b_ref, tok_ref, own, gb_ref)
        dw_ref[...] = jnp.dot(ga_ref[...], hn_a_ref[...], preferred_element_type=jnp.float32) + jnp.dot(gb_ref[...], hn_b_ref[...], preferred_element_type=jnp.float32)

    @pl.when(i >= FIRST)
    def _():
        own_part(g_out_ref)


def second_kernel(vocab, hn_a_ref, hn_b_ref, hnt_b_ref, w_ref, tok_ref, g_in_ref, dw_in_ref, dw_ref, wz_ref, gb_ref):
    i = pl.program_id(0)
    own = hnt_b_ref.shape[1]
    zero_tail(vocab, w_ref, wz_ref, i == pl.num_programs(0) - 1)
    softmax_grad(i + FIRST, wz_ref, hnt_b_ref, tok_ref, own, gb_ref)
    dw_ref[...] = jnp.dot(g_in_ref[...], hn_a_ref[...], preferred_element_type=jnp.float32) + jnp.dot(gb_ref[...], hn_b_ref[...], preferred_element_type=jnp.float32)


def full(shape):
    return pl.BlockSpec(shape, lambda i: (0,) * len(shape))


def solution(mesh):
    dp, vp = mesh.shape['dp'], mesh.shape['vp']

    def local(h_loc, norm_scale, w_loc, tgt_loc, wt_loc):
        own, width = h_loc.shape
        vocab = w_loc.shape[1]
        tokens = dp * own
        steps = pl.cdiv(vocab, BLOCK_V)
        me = lax.axis_index('vp')
        my_dp = lax.axis_index('dp')
        swap_dp = [(0, 1), (1, 0)]
        w_t = w_loc.T

        h_own = h_loc.astype(jnp.float32)
        h_oth = lax.ppermute(h_own, 'dp', swap_dp)
        tgt_oth = lax.ppermute(tgt_loc, 'dp', swap_dp)
        wt_oth = lax.ppermute(wt_loc, 'dp', swap_dp)

        def rstd(h):
            return lax.rsqrt(jnp.mean(h * h, axis=-1, keepdims=True) + EPS)

        r_own = rstd(h_own)
        hn_own = (h_own * r_own * norm_scale).astype(jnp.bfloat16)
        hnt_own = hn_own.T

        params = pltpu.CompilerParams(dimension_semantics=('arbitrary',), vmem_limit_bytes=60 * 2**20)
        unit = 2 * own * width * vocab
        st = pl.pallas_call(
            functools.partial(stats_kernel, vocab),
            grid=(steps,),
            in_specs=[full((width, own)), pl.BlockSpec((BLOCK_V, width), lambda i: (i, 0))],
            out_specs=full((2, own)),
            out_shape=jax.ShapeDtypeStruct((2, own), jnp.float32),
            scratch_shapes=[pltpu.VMEM((SUB, own), jnp.float32)] * 2,
            compiler_params=params,
            cost_estimate=pl.CostEstimate(flops=unit, bytes_accessed=2 * width * vocab, transcendentals=own * vocab),
            name='stats',
        )(hnt_own, w_t)
        h_oth, tgt_oth, wt_oth, st = lax.optimization_barrier((h_oth, tgt_oth, wt_oth, st))
        stats = lax.all_gather(st, ('dp', 'vp')).reshape(dp, vp, 2, own)
        top = jnp.max(stats[:, :, 0], axis=1)
        log_norm = top + jnp.log(jnp.sum(stats[:, :, 1] * jnp.exp(stats[:, :, 0] - top[:, None]), axis=1))
        w_total = jnp.sum(wt_loc) + jnp.sum(wt_oth)
        log_own = lax.dynamic_index_in_dim(log_norm, my_dp, 0, keepdims=False)
        log_oth = lax.dynamic_index_in_dim(log_norm, 1 - my_dp, 0, keepdims=False)

        hn_oth = (h_oth * rstd(h_oth) * norm_scale).astype(jnp.bfloat16)
        hnt_oth = hn_oth.T
        coef = jnp.concatenate([wt_loc, wt_oth]) / w_total
        lp = jnp.concatenate([log_own, log_oth]) - jnp.log(coef)
        rel = (jnp.concatenate([tgt_loc, tgt_oth]) - me * vocab).astype(jnp.float32)
        tok = jnp.broadcast_to(jnp.stack([lp, coef, rel])[:, None, :], (3, SUB, tokens)).reshape(3 * SUB, tokens)

        dw_shape = jax.ShapeDtypeStruct((vocab, width), jnp.float32)
        second = steps - FIRST
        dw_t, x, g_own = pl.pallas_call(
            functools.partial(first_kernel, vocab),
            grid=(steps,),
            in_specs=[full((own, width)), full((own, width)), full((width, own)), full((width, own)),
                      pl.BlockSpec((BLOCK_V, width), lambda i: (i, 0)), full((3 * SUB, tokens))],
            out_specs=[pl.BlockSpec((BLOCK_V, width), lambda i: (jnp.minimum(i, FIRST - 1), 0)), full((width + SUB, own)),
                       pl.BlockSpec((BLOCK_V, own), lambda i: (jnp.maximum(i - FIRST, 0), 0))],
            out_shape=[dw_shape, jax.ShapeDtypeStruct((width + SUB, own), jnp.float32), jax.ShapeDtypeStruct((second * BLOCK_V, own), jnp.bfloat16)],
            scratch_shapes=[pltpu.VMEM((BLOCK_V, width), jnp.bfloat16), pltpu.VMEM((BLOCK_V, own), jnp.bfloat16), pltpu.VMEM((BLOCK_V, own), jnp.bfloat16)],
            compiler_params=params,
            cost_estimate=pl.CostEstimate(flops=unit * (2 * steps + 3 * FIRST) // steps, bytes_accessed=4 * width * vocab, transcendentals=2 * own * vocab),
            name='grads_first',
        )(hn_own, hn_oth, hnt_own, hnt_oth, w_t, tok)

        hr = h_own * r_own
        ds_part = jnp.sum(x[:width] * hr.T, axis=1)
        zt_part = wt_loc * jnp.sum(x[width:], axis=0)
        extra = jnp.stack([jnp.concatenate([ds_part, jnp.zeros((own - width,), jnp.float32)]), zt_part])
        x = x.at[width:width + 2].set(extra)
        x = lax.psum(x, 'vp')

        dw_t = pl.pallas_call(
            functools.partial(second_kernel, vocab),
            grid=(second,),
            in_specs=[full((own, width)), full((own, width)), full((width, own)),
                      pl.BlockSpec((BLOCK_V, width), lambda i: (i + FIRST, 0)), full((3 * SUB, tokens)),
                      pl.BlockSpec((BLOCK_V, own), lambda i: (i, 0)), pl.BlockSpec(memory_space=pl.ANY)],
            out_specs=pl.BlockSpec((BLOCK_V, width), lambda i: (i + FIRST, 0)),
            out_shape=dw_shape,
            scratch_shapes=[pltpu.VMEM((BLOCK_V, width), jnp.bfloat16), pltpu.VMEM((BLOCK_V, own), jnp.bfloat16)],
            input_output_aliases={6: 0},
            compiler_params=params,
            cost_estimate=pl.CostEstimate(flops=unit * 3 * second // steps, bytes_accessed=4 * width * vocab, transcendentals=own * vocab),
            name='grads_second',
        )(hn_own, hn_oth, hnt_oth, w_t, tok, g_own, dw_t)

        mine = x[width:width + 2]
        both = mine + lax.ppermute(mine, 'dp', swap_dp)
        dhn = x[:width].T
        a = jnp.sum(dhn * norm_scale * h_own, axis=-1, keepdims=True)
        dh = r_own * norm_scale * dhn - h_own * (r_own * r_own * r_own) * (a / width)
        log_sum = jnp.sum(wt_loc * log_own) + jnp.sum(wt_oth * log_oth)
        loss = (log_sum - jnp.sum(both[1])) / w_total
        return loss, dh.astype(jnp.bfloat16), dw_t.T, both[0, :width]

    return jax.shard_map(local, mesh=mesh, in_specs=(P('dp', None), P(None), P(None, 'vp'), P('dp'), P('dp')), out_specs=(P(), P('dp', None), P(None, 'vp'), P(None)), check_vma=False)
```

```python
import functools

import jax
import jax.numpy as jnp
from jax import lax
from jax.experimental import pallas as pl
from jax.experimental.pallas import tpu as pltpu
from jax.sharding import PartitionSpec as P

EPS = 1e-6
SUB = 8
BLOCK_V = 1536
CHUNK = 512
GCHUNK = 512
MAX_SUM = 1e18
TN = (((0,), (0,)), ((), ()))
NT = (((1,), (1,)), ((), ()))


def last_rows(vocab):
    return vocab - (vocab - 1) // BLOCK_V * BLOCK_V


def stats_kernel(vocab, hnt_ref, w_ref, out_ref, z_ref, m_ref, s_ref, s_new_ref):
    i = pl.program_id(0)
    last = pl.num_programs(0) - 1
    tokens = hnt_ref.shape[1]

    @pl.when(i == 0)
    def _():
        z = jnp.dot(w_ref[:CHUNK, :], hnt_ref[...], preferred_element_type=jnp.float32)
        m_ref[...] = jnp.broadcast_to(jnp.max(z, axis=0, keepdims=True), m_ref.shape)
        s_ref[...] = jnp.zeros(s_ref.shape, jnp.float32)

    def exact(rows):
        for c in range(0, tokens, CHUNK):
            cols = pl.ds(c, CHUNK)
            z = jnp.dot(w_ref[:rows, :], hnt_ref[:, cols], preferred_element_type=jnp.float32)
            z = z.reshape(rows // SUB, SUB, CHUNK)
            m_old = m_ref[:, cols]
            m_new = jnp.maximum(m_old, jnp.max(z, axis=0))
            s_ref[:, cols] = s_ref[:, cols] * jnp.exp(m_old - m_new) + jnp.sum(jnp.exp(z - m_new[None]), axis=0)
            m_ref[:, cols] = m_new

    @pl.when(i < last)
    def _():
        largest = []
        for c in range(0, tokens, CHUNK):
            cols = pl.ds(c, CHUNK)
            z = jnp.dot(w_ref[...], hnt_ref[:, cols], preferred_element_type=jnp.float32)
            z_ref[:, cols] = z
            shifted = z.reshape(BLOCK_V // SUB, SUB, CHUNK) - m_ref[:, cols][None]
            total = s_ref[:, cols] + jnp.sum(jnp.exp(shifted), axis=0)
            largest.append(jnp.max(total))
            s_new_ref[:, cols] = total
        safe = functools.reduce(jnp.maximum, largest) <= MAX_SUM

        @pl.when(safe)
        def _():
            s_ref[...] = s_new_ref[...]

        @pl.when(jnp.logical_not(safe))
        def _():
            exact(BLOCK_V)

    @pl.when(i == last)
    def _():
        exact(last_rows(vocab))
        top = jnp.max(m_ref[...], axis=0, keepdims=True)
        out_ref[0:1, :] = top
        out_ref[1:2, :] = jnp.sum(s_ref[...] * jnp.exp(m_ref[...] - top), axis=0, keepdims=True)


def softmax_grad(z, step, tok_ref, toks):
    shape = (z.shape[0] // SUB, SUB, z.shape[1])
    z = z.reshape(shape)
    first_row = (lax.broadcasted_iota(jnp.int32, shape, 0) * SUB).astype(jnp.float32)
    row0 = (lax.broadcasted_iota(jnp.int32, shape[1:], 0) + step * BLOCK_V).astype(jnp.float32)
    hit = (tok_ref[2 * SUB:, toks] - row0)[None] == first_row
    g = jnp.exp(z - tok_ref[:SUB, toks][None]) - jnp.where(hit, tok_ref[SUB:2 * SUB, toks][None], 0.0)
    picked = jnp.sum(jnp.where(hit, z, 0.0), axis=0)
    return g.reshape(shape[0] * SUB, shape[2]).astype(jnp.bfloat16), picked


def other_grad(step, rows, w_ref, hnt_ref, tok_ref, g_ref):
    own = hnt_ref.shape[1]
    for c in range(0, own, GCHUNK):
        cols = pl.ds(c, GCHUNK)
        z = jnp.dot(w_ref[:rows, :], hnt_ref[:, cols], preferred_element_type=jnp.float32)
        g_ref[:rows, cols] = softmax_grad(z, step, tok_ref, pl.ds(own + c, GCHUNK))[0]


def weight_grad(rows, ga_ref, gb_ref, hnt_a_ref, hnt_b_ref):
    return (lax.dot_general(ga_ref[:rows, :], hnt_a_ref[...], NT, preferred_element_type=jnp.float32)
            + lax.dot_general(gb_ref[:rows, :], hnt_b_ref[...], NT, preferred_element_type=jnp.float32))


def first_kernel(vocab, first, hnt_a_ref, hnt_b_ref, w_ref, z_ref, tok_ref, dw_ref, x_ref, g_out_ref, ga_ref, gb_ref):
    i = pl.program_id(0)
    last = pl.num_programs(0) - 1
    width, own = hnt_a_ref.shape

    @pl.when(i == 0)
    def _():
        x_ref[...] = jnp.zeros(x_ref.shape, jnp.float32)

    def own_part(rows, g_ref, saved=False):
        for c in range(0, own, GCHUNK):
            cols = pl.ds(c, GCHUNK)
            z = z_ref[:, cols] if saved else jnp.dot(w_ref[:rows, :], hnt_a_ref[:, cols], preferred_element_type=jnp.float32)
            g, picked = softmax_grad(z, i, tok_ref, cols)
            g_ref[:rows, cols] = g
            x_ref[width:, cols] += picked
            x_ref[:width, cols] += lax.dot_general(w_ref[:rows, :], g, TN, preferred_element_type=jnp.float32)

    @pl.when(i < first)
    def _():
        own_part(BLOCK_V, ga_ref, saved=True)
        other_grad(i, BLOCK_V, w_ref, hnt_b_ref, tok_ref, gb_ref)
        dw_ref[...] = weight_grad(BLOCK_V, ga_ref, gb_ref, hnt_a_ref, hnt_b_ref)

    @pl.when(jnp.logical_and(i >= first, i < last))
    def _():
        own_part(BLOCK_V, g_out_ref)

    @pl.when(i == last)
    def _():
        own_part(last_rows(vocab), g_out_ref)


def second_kernel(vocab, first, hnt_a_ref, hnt_b_ref, w_ref, tok_ref, ga_ref, dw_in_ref, dw_ref, gb_ref):
    i = pl.program_id(0)
    last = pl.num_programs(0) - 1

    def block(rows):
        other_grad(i + first, rows, w_ref, hnt_b_ref, tok_ref, gb_ref)
        dw_ref[:rows, :] = weight_grad(rows, ga_ref, gb_ref, hnt_a_ref, hnt_b_ref)

    @pl.when(i < last)
    def _():
        block(BLOCK_V)

    @pl.when(i == last)
    def _():
        block(last_rows(vocab))


def hidden_grad_kernel(x_ref, h_ref, scale_ref, dh_ref):
    width = h_ref.shape[1]
    h = h_ref[...].astype(jnp.float32)
    r = lax.rsqrt(jnp.mean(h * h, axis=-1, keepdims=True) + EPS)
    sd = scale_ref[...] * x_ref[:width, :].T
    a = jnp.sum(sd * h, axis=-1, keepdims=True)
    dh_ref[...] = (r * sd - h * (r * r * r) * (a / width)).astype(jnp.bfloat16)


def full(shape):
    return pl.BlockSpec(shape, lambda i: (0,) * len(shape))


def solution(mesh):
    dp, vp = mesh.shape['dp'], mesh.shape['vp']

    def local(h_loc, norm_scale, w_loc, tgt_loc, wt_loc):
        own, width = h_loc.shape
        vocab = w_loc.shape[1]
        tokens = dp * own
        steps = pl.cdiv(vocab, BLOCK_V)
        first = (steps + 1) // 2
        second = steps - first
        me = lax.axis_index('vp')
        my_dp = lax.axis_index('dp')
        swap_dp = [(0, 1), (1, 0)]
        w_t = w_loc.T

        scale = norm_scale[None, :]
        whole = pltpu.CompilerParams(vmem_limit_bytes=40 * 2**20)
        h_own = h_loc.astype(jnp.float32)
        h_oth = lax.ppermute(h_own, 'dp', swap_dp)
        tgt_oth = lax.ppermute(tgt_loc, 'dp', swap_dp)
        wt_oth = lax.ppermute(wt_loc, 'dp', swap_dp)

        def rstd(h):
            return lax.rsqrt(jnp.mean(h * h, axis=-1, keepdims=True) + EPS)

        hr_own = h_own * rstd(h_own)
        hnt_own = (hr_own * norm_scale).astype(jnp.bfloat16).T

        params = pltpu.CompilerParams(dimension_semantics=('arbitrary',), vmem_limit_bytes=60 * 2**20)
        unit = 2 * own * width * vocab
        st, z_own = pl.pallas_call(
            functools.partial(stats_kernel, vocab),
            grid=(steps,),
            in_specs=[full((width, own)), pl.BlockSpec((BLOCK_V, width), lambda i: (i, 0))],
            out_specs=[full((2, own)), pl.BlockSpec((BLOCK_V, own), lambda i: (jnp.minimum(i, first), 0))],
            out_shape=[jax.ShapeDtypeStruct((2, own), jnp.float32), jax.ShapeDtypeStruct(((first + 1) * BLOCK_V, own), jnp.float32)],
            scratch_shapes=[pltpu.VMEM((SUB, own), jnp.float32)] * 3,
            compiler_params=params,
            cost_estimate=pl.CostEstimate(flops=unit, bytes_accessed=(2 * width + 2 * own) * vocab, transcendentals=own * vocab),
            name='stats',
        )(hnt_own, w_t)
        h_oth, tgt_oth, wt_oth, st = lax.optimization_barrier((h_oth, tgt_oth, wt_oth, st))
        stats = lax.all_gather(st, ('dp', 'vp')).reshape(dp, vp, 2, own)
        top = jnp.max(stats[:, :, 0], axis=1)
        log_norm = top + jnp.log(jnp.sum(stats[:, :, 1] * jnp.exp(stats[:, :, 0] - top[:, None]), axis=1))
        w_total = jnp.sum(wt_loc) + jnp.sum(wt_oth)
        log_own = lax.dynamic_index_in_dim(log_norm, my_dp, 0, keepdims=False)
        log_oth = lax.dynamic_index_in_dim(log_norm, 1 - my_dp, 0, keepdims=False)

        hn_oth = (h_oth * rstd(h_oth) * norm_scale).astype(jnp.bfloat16)
        hnt_oth = hn_oth.T
        coef = jnp.concatenate([wt_loc, wt_oth]) / w_total
        lp = jnp.concatenate([log_own, log_oth]) - jnp.log(coef)
        rel = jnp.concatenate([tgt_loc, tgt_oth]) - me * vocab
        rel = jnp.where(rel < vocab, rel, -1).astype(jnp.float32)
        tok = jnp.broadcast_to(jnp.stack([lp, coef, rel])[:, None, :], (3, SUB, tokens)).reshape(3 * SUB, tokens)

        dw_shape = jax.ShapeDtypeStruct((vocab, width), jnp.float32)
        dw_t, x, g_own = pl.pallas_call(
            functools.partial(first_kernel, vocab, first),
            grid=(steps,),
            in_specs=[full((width, own)), full((width, own)), pl.BlockSpec((BLOCK_V, width), lambda i: (i, 0)),
                      pl.BlockSpec((BLOCK_V, own), lambda i: (jnp.minimum(i, first - 1), 0)), full((3 * SUB, tokens))],
            out_specs=[pl.BlockSpec((BLOCK_V, width), lambda i: (jnp.minimum(i, first - 1), 0)), full((width + SUB, own)),
                       pl.BlockSpec((BLOCK_V, own), lambda i: (jnp.maximum(i - first, 0), 0))],
            out_shape=[dw_shape, jax.ShapeDtypeStruct((width + SUB, own), jnp.float32), jax.ShapeDtypeStruct((second * BLOCK_V, own), jnp.bfloat16)],
            scratch_shapes=[pltpu.VMEM((BLOCK_V, own), jnp.bfloat16)] * 2,
            compiler_params=params,
            cost_estimate=pl.CostEstimate(flops=unit * (2 * steps + 2 * first) // steps, bytes_accessed=(4 * width + 2 * own) * vocab, transcendentals=2 * own * vocab),
            name='grads_first',
        )(hnt_own, hnt_oth, w_t, z_own, tok)

        ds_part = jnp.sum(x[:width] * hr_own.T, axis=1)
        zt_part = wt_loc * jnp.sum(x[width:], axis=0)
        extra = jnp.stack([jnp.concatenate([ds_part, jnp.zeros((own - width,), jnp.float32)]), zt_part])
        x = x.at[width:width + 2].set(extra)
        x = lax.psum(x, 'vp')

        dw_t = pl.pallas_call(
            functools.partial(second_kernel, vocab, first),
            grid=(second,),
            in_specs=[full((width, own)), full((width, own)),
                      pl.BlockSpec((BLOCK_V, width), lambda i: (i + first, 0)), full((3 * SUB, tokens)),
                      pl.BlockSpec((BLOCK_V, own), lambda i: (i, 0)), pl.BlockSpec(memory_space=pl.ANY)],
            out_specs=pl.BlockSpec((BLOCK_V, width), lambda i: (i + first, 0)),
            out_shape=dw_shape,
            scratch_shapes=[pltpu.VMEM((BLOCK_V, own), jnp.bfloat16)],
            input_output_aliases={5: 0},
            compiler_params=params,
            cost_estimate=pl.CostEstimate(flops=unit * 3 * second // steps, bytes_accessed=4 * width * vocab, transcendentals=own * vocab),
            name='grads_second',
        )(hnt_own, hnt_oth, w_t, tok, g_own, dw_t)

        x, dw_t = lax.optimization_barrier((x, dw_t))
        mine = x[width:width + 2]
        both = mine + lax.ppermute(mine, 'dp', swap_dp)
        dh = pl.pallas_call(
            hidden_grad_kernel,
            out_shape=jax.ShapeDtypeStruct((own, width), jnp.bfloat16),
            compiler_params=whole,
            name='hidden_grad',
        )(x, h_loc, scale)
        log_sum = jnp.sum(wt_loc * log_own) + jnp.sum(wt_oth * log_oth)
        loss = (log_sum - jnp.sum(both[1])) / w_total
        return loss, dh, dw_t.T, both[0, :width]

    return jax.shard_map(local, mesh=mesh, in_specs=(P('dp', None), P(None), P(None, 'vp'), P('dp'), P('dp')), out_specs=(P(), P('dp', None), P(None, 'vp'), P(None)), check_vma=False)
```
